32 devices in a mesh: row: 2 (over y), tm: 16 (over z, x, core).
Axes of the slice: x: 2, y: 2, z: 4, core: 2. Of those that a mesh axis runs over, the one named last changes fastest.
Arguments:
- occ_factor: float32 [32, 512, 2048], P('tm', 'row'), may hold values from -0.077339804 to 0.077339804
- vir_factor: float32 [32, 512, 2048], P('tm', 'row'), may hold values from -0.077339804 to 0.077339804
- eps_basis: float32 [512, 1024], P('row'), may hold values from -0.25 to 0.25
Outputs:
- screened: float32 [32, 1024, 1024], P('tm', 'row')
The draws below stay inside these ranges and needn't reach their ends.
All inputs are finite; a program needn't handle non-finite values.
Results may differ from the reference program's by a relative error of at most 0.000075.
Values sent between devices are 32-bit elements; how exact they have to be, the bound alone decides.
No kernel may reach another device: no remote copies, remote signals or barrier semaphores. Data moves between devices by JAX's collectives and lax.ppermute only.
A program may use at most 128 MiB of HBM per device.

```python
import jax
import jax.numpy as jnp
from jax import lax

NOCC = 2048
NVIR = 2048
NEPS = 1024
NT = 32
NAUX = 512


def factor_draw(key, width, salt):
    common = jax.random.normal(jax.random.fold_in(key, salt + 1), (NT, 1, width), jnp.float32)
    private = jax.random.normal(jax.random.fold_in(key, salt + 2), (NT, NAUX, width), jnp.float32)
    values = jnp.clip((common + private) * 0.7071, -3.5, 3.5)
    return (values / jnp.sqrt(jnp.float32(width))).astype(jnp.float32)


def draw_occ_factor(key, part):
    return factor_draw(key, NOCC, 110)


def draw_vir_factor(key, part):
    return factor_draw(key, NVIR, 220)


def steps_of(own_key, extent, split, low, high):
    def one(dim, shards_of):
        steps = jax.random.uniform(jax.random.fold_in(jax.random.fold_in(own_key, 6), dim), (shards_of,), jnp.float32, low / len(split), high / len(split))
        return jnp.repeat(jnp.exp(steps), extent[dim] // shards_of).reshape((-1,) + (1,) * (len(extent) - dim - 1))

    loudness = one(*split[0])
    for cut in split[1:]:
        loudness = loudness * one(*cut)
    return loudness


def centred(rng, shape, deviation, reach, shards=(), held_as=jnp.bfloat16):
    result = deviation * jax.random.normal(rng, shape, jnp.float32)
    if shards:
        result = result * steps_of(rng, shape, shards, -0.22, 0.18)
    return jnp.clip(result, -reach, reach).astype(held_as)


def setup_inputs(seed: int = 0) -> dict:
    seeds = jax.random.split(jax.random.key(seed), 4)
    occ_factor = draw_occ_factor(jax.random.fold_in(seeds[3], 71), 0)
    vir_factor = draw_vir_factor(jax.random.fold_in(seeds[3], 71), 0)
    eps_basis = centred(seeds[2], (NAUX, NEPS), NAUX ** -0.5, 0.25, ((0, 2),), jnp.float32)
    return {"occ_factor": occ_factor, "vir_factor": vir_factor, "eps_basis": eps_basis}


highest = lax.Precision.HIGHEST

def cosine_table(length):
    freq_index = jnp.arange(length, dtype=jnp.float32)[:, None]
    time_index = jnp.arange(length, dtype=jnp.float32)[None, :]
    table = jnp.cos(jnp.pi * freq_index * (time_index + 0.5) / length) * jnp.sqrt(2.0 / length)
    return jnp.where(freq_index == 0, table * jnp.sqrt(0.5), table)

def reference(occ_factor, vir_factor, eps_basis):

    def one_time(pair):
        occ_slice, vir_slice = pair
        occ_green = jnp.dot(occ_slice, occ_slice.T, precision=highest, preferred_element_type=jnp.float32)
        vir_green = jnp.dot(vir_slice, vir_slice.T, precision=highest, preferred_element_type=jnp.float32)
        polar = occ_green * vir_green
        return jnp.dot(polar, eps_basis, precision=highest, preferred_element_type=jnp.float32)
    projected = lax.map(one_time, (occ_factor, vir_factor))
    table = cosine_table(NT)
    spectrum = jnp.einsum('kt,tpe->kpe', table, projected, precision=highest)

    def project_left(block):
        return jnp.dot(eps_basis.T, block, precision=highest, preferred_element_type=jnp.float32)
    return lax.map(project_left, spectrum)
```

```python
import jax
import jax.numpy as jnp
from jax import lax
from jax.sharding import PartitionSpec as P

highest = lax.Precision.HIGHEST
high = lax.Precision.HIGH


def cosine_table(length):
    freq_index = jnp.arange(length, dtype=jnp.float32)[:, None]
    time_index = jnp.arange(length, dtype=jnp.float32)[None, :]
    table = jnp.cos(jnp.pi * freq_index * (time_index + 0.5) / length) * jnp.sqrt(2.0 / length)
    return jnp.where(freq_index == 0, table * jnp.sqrt(0.5), table)


def pair_tiles(own_occ, own_vir, far_occ, far_vir):
    occ_tile = jnp.einsum("trn,tkn->trk", own_occ, far_occ, precision=highest)
    vir_tile = jnp.einsum("trn,tkn->trk", own_vir, far_vir, precision=highest)
    return occ_tile * vir_tile


def any_rows(occ_factor, vir_factor, eps_basis):
    local_times = occ_factor.shape[0]
    time_total = local_times * lax.axis_size("tm")
    table = cosine_table(time_total)
    far_occ = lax.all_gather(occ_factor, "row", axis=1, tiled=True)
    far_vir = lax.all_gather(vir_factor, "row", axis=1, tiled=True)
    polar = pair_tiles(occ_factor, vir_factor, far_occ, far_vir)
    frequency_block = jnp.einsum(
        "kt,tic->kic",
        table,
        lax.all_to_all(polar, "tm", split_axis=2, concat_axis=0, tiled=True),
        precision=highest,
    )
    spectrum = lax.all_to_all(frequency_block, "tm", split_axis=0, concat_axis=2, tiled=True)
    full_basis = lax.all_gather(eps_basis, "row", axis=0, tiled=True)
    projected = jnp.einsum("fra,ae->fre", spectrum, full_basis, precision=highest)
    partial_terms = jnp.einsum("re,fro->feo", eps_basis, projected, precision=highest)
    return lax.psum_scatter(partial_terms, "row", scatter_dimension=1, tiled=True)


def two_rows(occ_factor, vir_factor, eps_basis):
    local_times, rows, depth = occ_factor.shape
    tm = lax.axis_size("tm")
    basis = eps_basis.shape[1]
    r = lax.axis_index("row")
    j = lax.axis_index("tm")
    swap = [(0, 1), (1, 0)]
    times = local_times * tm
    devices = 2 * tm
    table = cosine_table(times)

    piece = rows // tm
    far_piece = lax.ppermute(lax.dynamic_slice_in_dim(eps_basis, j * piece, piece, 0), "row", swap)

    chunks = 4
    step = rows // chunks

    def travel(factor):
        return [
            lax.ppermute(
                lax.dynamic_slice(factor, (1 - r, c * step, 0), (1, step, depth))[0], "row", swap
            )
            for c in range(chunks)
        ]

    far_occ = travel(occ_factor)
    far_vir = travel(vir_factor)

    far_basis = lax.all_to_all(
        jnp.broadcast_to(far_piece[None], (tm, piece, basis)), "tm", 0, 0, tiled=True
    ).reshape(rows, basis)

    half = rows // 2
    own_green = jnp.einsum("trn,tkn->trk", occ_factor, occ_factor, precision=high)
    own_green = own_green * jnp.einsum("trn,tkn->trk", vir_factor, vir_factor, precision=high)
    tiles = jnp.stack(
        [own_green[:, :half, :half], own_green[:, half:, :half], own_green[:, half:, half:]], 1
    )
    tall = 3 * half // tm
    packed = tiles.reshape(local_times, tm, tall, half).transpose(1, 0, 2, 3)
    packed = lax.all_to_all(packed, "tm", 0, 0, tiled=True).reshape(times, tall, half)
    packed = jnp.einsum("kt,tic->kic", table, packed, precision=highest)
    packed = lax.all_to_all(
        packed.reshape(tm, local_times, tall, half), "tm", 0, 0, tiled=True
    )
    own_tiles = packed.transpose(1, 0, 2, 3).reshape(local_times, 3, half, half)
    far_tiles = lax.ppermute(own_tiles, "row", swap)

    def whole(t):
        top = jnp.concatenate([t[:, 0], t[:, 1].transpose(0, 2, 1)], 2)
        return jnp.concatenate([top, jnp.concatenate([t[:, 1], t[:, 2]], 2)], 1)

    def across(far, factor):
        own = lax.dynamic_index_in_dim(factor, r, 0, keepdims=False)
        return jnp.concatenate(
            [jnp.einsum("kn,rn->kr", f, own, precision=high) for f in far], 0
        )

    cross = across(far_occ, occ_factor) * across(far_vir, vir_factor)
    cross = jnp.where(r == 0, cross.T, cross)
    strip = rows // devices
    cross = lax.all_to_all(cross.reshape(devices, strip, rows), ("row", "tm"), 0, 0, tiled=True)
    by_source = table.reshape(times, tm, 2).transpose(0, 2, 1).reshape(times, times)
    cross = jnp.einsum("ks,sic->kic", by_source, cross, precision=highest)
    cross = cross.reshape(1, tm, local_times, strip, rows)
    cross = jnp.broadcast_to(cross, (2, tm, local_times, strip, rows))
    cross = lax.all_to_all(
        cross.reshape(devices, local_times, strip, rows), ("row", "tm"), 0, 0, tiled=True
    )
    cross = cross.transpose(1, 0, 2, 3).reshape(local_times, rows, rows)
    cross = jnp.where(r == 0, cross, cross.transpose(0, 2, 1))

    out_rows = basis // 2
    own_left = lax.dynamic_slice_in_dim(eps_basis, r * out_rows, out_rows, 1)
    far_left = lax.dynamic_slice_in_dim(far_basis, r * out_rows, out_rows, 1)
    own_part = jnp.einsum("ae,fab->feb", own_left, whole(own_tiles), precision=high)
    own_part = own_part + jnp.einsum("ae,fba->feb", far_left, cross, precision=high)
    far_part = jnp.einsum("ae,fab->feb", far_left, whole(far_tiles), precision=high)
    far_part = far_part + jnp.einsum("ae,fab->feb", own_left, cross, precision=high)
    both = jnp.concatenate([own_part, far_part], 2)
    return jnp.einsum(
        "fea,ao->feo", both, jnp.concatenate([eps_basis, far_basis], 0), precision=high
    )


def on_device(occ_factor, vir_factor, eps_basis):
    local_times, rows, _ = occ_factor.shape
    tm = lax.axis_size("tm")
    fits = lax.axis_size("row") == 2 and local_times == 2
    fits = fits and rows % (2 * tm) == 0 and eps_basis.shape[1] % 2 == 0 and 3 * rows % (2 * tm) == 0
    if fits:
        return two_rows(occ_factor, vir_factor, eps_basis)
    return any_rows(occ_factor, vir_factor, eps_basis)


def solution(mesh):
    placed = (P("tm", "row", None), P("tm", "row", None), P("row", None))
    return jax.shard_map(
        on_device, mesh=mesh, in_specs=placed, out_specs=P("tm", "row", None), check_vma=False
    )
```
